32 devices in a mesh: section: 2 (over x), lat: 4 (over y, core), lon: 4 (over z).
Axes of the slice: x: 2, y: 2, z: 4, core: 2. Of those that a mesh axis runs over, the one named last changes fastest.
Arguments:
- fields_in: bfloat16 [4, 96, 64, 512], P('section', None, 'lat', 'lon'), may hold values from -6 to 6
- plan: int32 [4], replicated, may hold values from 0 to 3, as said below
- in_proj: bfloat16 [64, 96], replicated, may hold values from -0.625 to 0.625
- enc_conv: bfloat16 [9, 64, 64], replicated, may hold values from -0.25 to 0.25
- down_conv: bfloat16 [9, 128, 64], replicated, may hold values from -0.25 to 0.25
- mid_conv: bfloat16 [9, 128, 128], replicated, may hold values from -0.1875 to 0.1875
- up_proj: bfloat16 [64, 128], replicated, may hold values from -0.5 to 0.5
- unite_conv: bfloat16 [9, 64, 128], replicated, may hold values from -0.1875 to 0.1875
- out_proj: bfloat16 [96, 64], replicated, may hold values from -0.75 to 0.75
Outputs:
- corrected: bfloat16 [4, 96, 64, 512], P('section', None, 'lat', 'lon')
The draws below stay inside these ranges and needn't reach their ends.
Inputs may be any that keep to these rules, and one draw needn't show every extreme that they name: `plan`: each micro-batch appears once; the first turn takes one of the last 2 micro-batches and the last turn one of the first 2.
All inputs are finite; a program needn't handle non-finite values.
Results may differ from the reference program's by a relative error of at most 0.0072.
Values may be sent and summed in bfloat16 or wider, within the bound.
No kernel may reach another device: no remote copies, remote signals or barrier semaphores. Data moves between devices by JAX's collectives and lax.ppermute only.
A program may use at most 64 MiB of HBM per device.

```python
import jax
import jax.numpy as jnp
from jax import lax

VARS = 96
C0 = 64
C1 = 128
MICRO = 4
LAT = 64
LON = 512


def draw_plan(key, part):
    half_count = MICRO // 2
    opening = jax.random.randint(jax.random.fold_in(key, 11), (), half_count, MICRO).astype(jnp.int32)
    closing = jax.random.randint(jax.random.fold_in(key, 12), (), 0, half_count).astype(jnp.int32)
    shuffled = jax.random.permutation(jax.random.fold_in(key, 13), MICRO).astype(jnp.int32)
    position = jnp.argsort(shuffled, stable=True).astype(jnp.int32)
    numbers = jnp.arange(MICRO, dtype=jnp.int32)
    taken = (numbers == opening) | (numbers == closing)
    scores = jnp.where(taken, jnp.int32(2 * MICRO), position)
    remaining = jnp.argsort(scores, stable=True).astype(jnp.int32)[:MICRO - 2]
    return jnp.concatenate([opening[None], remaining, closing[None]]).astype(jnp.int32)


def block_levels(rng, dims, pieces, low, largest):
    gain = 1.0
    for dim, blocks in pieces:
        steps = jax.random.uniform(jax.random.fold_in(jax.random.fold_in(rng, 6), dim), (blocks,), jnp.float32, low / len(pieces), largest / len(pieces))
        gain = gain * jnp.repeat(jnp.exp(steps), dims[dim] // blocks).reshape((-1,) + (1,) * (len(dims) - 1 - dim))
    return gain


def centred(key, shape, deviation, reach, split=(), held_as=jnp.bfloat16):
    factor_of = block_levels(key, shape, split, -0.22, 0.18) if split else 1.0
    values = jax.random.normal(key, shape, jnp.float32) * deviation * factor_of
    return jnp.minimum(jnp.maximum(values, -reach), reach).astype(held_as)


def setup_inputs(seed: int = 0) -> dict:
    keys = jax.random.split(jax.random.key(seed), 10)
    fields_in = centred(keys[0], (MICRO, VARS, LAT, LON), 1.0, 6.0, ((0, 2), (2, 4), (3, 4)))
    plan = draw_plan(jax.random.fold_in(keys[9], 71), 0)
    in_proj = centred(keys[2], (C0, VARS), VARS ** -0.5, 0.625)
    enc_conv = centred(keys[3], (9, C0, C0), (9 * C0) ** -0.5, 0.25)
    down_conv = centred(keys[4], (9, C1, C0), (9 * C0) ** -0.5, 0.25)
    mid_conv = centred(keys[5], (9, C1, C1), (9 * C1) ** -0.5, 0.1875)
    up_proj = centred(keys[6], (C0, C1), C1 ** -0.5, 0.5)
    unite_conv = centred(keys[7], (9, C0, 2 * C0), (18 * C0) ** -0.5, 0.1875)
    out_proj = centred(keys[8], (VARS, C0), C0 ** -0.5, 0.75)
    return {"fields_in": fields_in, "plan": plan, "in_proj": in_proj, "enc_conv": enc_conv, "down_conv": down_conv, "mid_conv": mid_conv, "up_proj": up_proj, "unite_conv": unite_conv, "out_proj": out_proj}


def convolve(source, kernel):
    channels, height, breadth = source.shape
    padded = jnp.pad(source, ((0, 0), (0, 0), (1, 1)), mode="wrap")
    padded = jnp.pad(padded, ((0, 0), (1, 1), (0, 0)))
    summed = jnp.zeros((kernel.shape[1], height * breadth), jnp.float32)
    for offset_row in range(3):
        for offset_col in range(3):
            window = padded[:, offset_row:offset_row + height, offset_col:offset_col + breadth].reshape(channels, height * breadth)
            summed = summed + jnp.dot(kernel[3 * offset_row + offset_col], window, preferred_element_type=jnp.float32)
    return summed.reshape(kernel.shape[1], height, breadth)


def encode(sample, in_proj, enc_conv, down_conv):
    variables, height, breadth = sample.shape
    stem_map = jax.nn.gelu(jnp.dot(in_proj, sample.reshape(variables, height * breadth), preferred_element_type=jnp.float32))
    stem_map = stem_map.astype(jnp.bfloat16).reshape(-1, height, breadth)
    skip_map = jax.nn.gelu(convolve(stem_map, enc_conv)).astype(jnp.bfloat16)
    pooled = skip_map.astype(jnp.float32).reshape(-1, height // 2, 2, breadth // 2, 2).mean(axis=(2, 4)).astype(jnp.bfloat16)
    deep_map = jax.nn.gelu(convolve(pooled, down_conv)).astype(jnp.bfloat16)
    return skip_map, deep_map


def decode(skip_map, deep_map, mid_conv, up_proj, unite_conv, out_proj):
    middle = (jax.nn.gelu(convolve(deep_map, mid_conv)) + deep_map.astype(jnp.float32)).astype(jnp.bfloat16)
    wide_ch, half_h, half_w = middle.shape
    lifted = jnp.dot(up_proj, middle.reshape(wide_ch, half_h * half_w), preferred_element_type=jnp.float32)
    lifted = lifted.astype(jnp.bfloat16).reshape(-1, half_h, half_w)
    enlarged = jnp.repeat(jnp.repeat(lifted, 2, axis=1), 2, axis=2)
    joined = jnp.concatenate([enlarged, skip_map], axis=0)
    merged = jax.nn.gelu(convolve(joined, unite_conv)).astype(jnp.bfloat16)
    narrow_ch, height, breadth = merged.shape
    result = jnp.dot(out_proj, merged.reshape(narrow_ch, height * breadth), preferred_element_type=jnp.float32)
    return result.astype(jnp.bfloat16).reshape(-1, height, breadth)


def reference(fields_in, plan, in_proj, enc_conv, down_conv, mid_conv, up_proj, unite_conv, out_proj):
    results = []
    for tick_num in range(MICRO):
        sample = lax.dynamic_index_in_dim(fields_in, plan[tick_num].astype(jnp.int32), 0, keepdims=False)
        skip_map, deep_map = encode(sample, in_proj, enc_conv, down_conv)
        results.append(decode(skip_map, deep_map, mid_conv, up_proj, unite_conv, out_proj))
    return jnp.stack(results)
```

```python
import jax
import jax.numpy as jnp
from jax import lax
from jax.experimental import pallas as pl
from jax.experimental.pallas import tpu as pltpu
from jax.sharding import PartitionSpec as P

BF = jnp.bfloat16
F32 = jnp.float32
HALO = 8


def gelu(x):
    inner = x * (0.7978845608028654 + 0.035677408136300125 * (x * x))
    half = 0.5 * x
    return half + half * jnp.tanh(inner)


def dot(a, b):
    return jnp.dot(a, b, preferred_element_type=F32)


def shift(x, by):
    n = x.shape[1]
    by = by % n
    if by == 0:
        return x
    return jnp.concatenate([x[:, by:], x[:, :by]], axis=1)


def swap_pairs(count, odd, periodic):
    pairs = []
    for low in range(1 if odd else 0, count, 2):
        high = low + 1
        if high >= count:
            if not periodic:
                continue
            high = 0
        pairs += [(low, high), (high, low)]
    return pairs


def stem_kernel(fields, w_in, stem, strip_x, strip_y, tall):
    samples, variables, height, breadth = fields.shape
    odd = lax.axis_index("lon") % 2
    for b in range(samples):
        tall[b] = fields[b].astype(F32)
        cols = []
        for i in range(height):
            cols.append(tall[b, :, i, :].astype(BF))
        picked = jnp.concatenate(cols, axis=1)
        full = gelu(dot(w_in[...], picked)).astype(BF)
        stem[b] = full
        left = jnp.concatenate([full[:, i * breadth : i * breadth + HALO] for i in range(height)], axis=1)
        right = jnp.concatenate(
            [full[:, (i + 1) * breadth - HALO : (i + 1) * breadth] for i in range(height)], axis=1
        )
        strip_x[b] = jnp.where(odd == 1, left, right)
        strip_y[b] = jnp.where(odd == 1, right, left)


def widen_kernel(breadth, stem, recv_x, recv_y, half_x, half_y):
    samples = stem.shape[0]
    height = stem.shape[2] // breadth
    half = height // 2
    lon_odd = lax.axis_index("lon") % 2
    lat_odd = lax.axis_index("lat") % 2
    for b in range(samples):
        full = stem[b]
        from_x, from_y = recv_x[b], recv_y[b]
        left = jnp.where(lon_odd == 1, from_x, from_y)
        right = jnp.where(lon_odd == 1, from_y, from_x)
        halves = []
        for first in (0, half):
            pieces = []
            for m in range(4):
                for k in range(half // 4):
                    i = first + 4 * k + m
                    pieces += [
                        left[:, i * HALO : (i + 1) * HALO],
                        full[:, i * breadth : (i + 1) * breadth],
                        right[:, i * HALO : (i + 1) * HALO],
                    ]
            halves.append(jnp.concatenate(pieces, axis=1))
        half_x[b] = jnp.where(lat_odd == 1, halves[0], halves[1])
        half_y[b] = jnp.where(lat_odd == 1, halves[1], halves[0])


def unet_kernel(
    which, per_section, lat_count, breadth, plan, own_x, own_y, recv_x, recv_y, w_enc, w_down, w_mid, w_up, w_unite,
    merged, quads, zz1, zz2, zz3, zz4, sems,
):
    pitch = breadth + 2 * HALO
    lat = lax.axis_index("lat")
    section = lax.axis_index("section")
    odd = lat % 2
    first_turn = plan[0] - per_section
    last_turn = plan[2 * per_section - 1]
    sample = jnp.where(section == 0, last_turn, first_turn)
    if which == 1:
        sample = 1 - sample
    copies = []
    for n, (source, slot) in enumerate(
        ((own_x, 2 - odd), (own_y, 1 + odd), (recv_x, 3 - 3 * odd), (recv_y, 3 * odd))
    ):
        copy = pltpu.make_async_copy(source.at[sample], quads.at[slot], sems.at[n])
        copy.start()
        copies.append(copy)
    for copy in copies:
        copy.wait()
    c0 = quads.shape[1]
    lanes = quads.shape[2]
    quarter = lanes // 4
    low_edge = lat == 0
    high_edge = lat == lat_count - 1

    def keep(width, low, high):
        lane = lax.broadcasted_iota(jnp.int32, (1, width), 1)
        drop = (low_edge & (lane < low)) | (high_edge & (lane >= high))
        return jnp.where(drop, 0.0, 1.0).astype(F32)

    full_keep = keep(lanes, quarter, lanes - quarter)
    planes = [
        jnp.concatenate([quads[s, :, m * quarter : (m + 1) * quarter] for s in range(4)], axis=1)
        for m in range(4)
    ]
    rows = [shift(planes[3], -pitch)] + planes + [shift(planes[0], pitch)]
    for j, row in enumerate(rows):
        base = j * 3 * c0
        zz1[base : base + c0] = shift(row, -1)
        zz1[base + c0 : base + 2 * c0] = row
        zz1[base + 2 * c0 : base + 3 * c0] = shift(row, 1)
    skip = []
    for q in range(2):
        out = dot(w_enc[...], zz1[2 * q * 3 * c0 : (2 * q + 4) * 3 * c0])
        out = (gelu(out) * full_keep).astype(BF)
        skip += [out[:c0], out[c0:]]

    blocks = -(-lanes // 256)
    spare = blocks * 256 - lanes
    to_lane = lax.broadcasted_iota(jnp.int32, (512, 128), 1)
    from_lane = lax.broadcasted_iota(jnp.int32, (512, 128), 0) % 256
    gather = jnp.where(from_lane // 2 == to_lane, 0.25, 0.0).astype(BF)
    stacked = []
    for h in range(2):
        pair = [
            jnp.concatenate([skip[2 * h + e], jnp.zeros((c0, spare), BF)], axis=1) if spare else skip[2 * h + e]
            for e in range(2)
        ]
        for t in range(blocks):
            stacked.append(
                jnp.concatenate([pair[0][:, 256 * t : 256 * (t + 1)], pair[1][:, 256 * t : 256 * (t + 1)]], axis=1)
            )
    small = dot(jnp.concatenate(stacked, axis=0), gather).astype(BF)
    pooled = [
        jnp.concatenate([small[(h * blocks + t) * c0 : (h * blocks + t + 1) * c0] for t in range(blocks)], axis=1)
        for h in range(2)
    ]
    half_lanes = 128 * blocks
    half_pitch = pitch // 2
    half_keep = keep(half_lanes, quarter // 2, (lanes - quarter) // 2)

    def halves(scratch, source):
        width = source[0].shape[0]
        for j, row in enumerate(
            (shift(source[1], -half_pitch), source[0], source[1], shift(source[0], half_pitch))
        ):
            base = j * 3 * width
            scratch[base : base + width] = shift(row, -1)
            scratch[base + width : base + 2 * width] = row
            scratch[base + 2 * width : base + 3 * width] = shift(row, 1)

    halves(zz2, pooled)
    deep = []
    for h in range(2):
        out = dot(w_down[...], zz2[h * 3 * c0 : (h + 3) * 3 * c0])
        deep.append((gelu(out) * half_keep).astype(BF))
    halves(zz3, deep)
    c1 = deep[0].shape[0]
    lifted = []
    for h in range(2):
        out = dot(w_mid[...], zz3[h * 3 * c1 : (h + 3) * 3 * c1])
        middle = (gelu(out) + deep[h].astype(F32)).astype(BF)
        lifted.append((dot(w_up[...], middle) * half_keep).astype(BF))
    wide_lane = lax.broadcasted_iota(jnp.int32, (128, 256), 1)
    thin_lane = lax.broadcasted_iota(jnp.int32, (128, 256), 0)
    spread = jnp.where(wide_lane // 2 == thin_lane, 1.0, 0.0).astype(BF)
    stacked = jnp.concatenate(
        [lifted[h][:, 128 * t : 128 * (t + 1)] for h in range(2) for t in range(blocks)], axis=0
    )
    large = dot(stacked, spread).astype(BF)
    raised = [
        jnp.concatenate([large[(h * blocks + t) * c0 : (h * blocks + t + 1) * c0] for t in range(blocks)], axis=1)
        for h in range(2)
    ]
    start = quarter // 128 * 128
    span = zz4.shape[1]
    lift_rows = [(raised[1], -pitch), (raised[0], 0), (raised[0], 0), (raised[1], 0), (raised[1], 0), (raised[0], pitch)]
    skip_rows = [(skip[3], -pitch)] + [(s, 0) for s in skip] + [(skip[0], pitch)]
    for j in range(6):
        for b in range(3):
            base = (3 * j + b) * 2 * c0
            row, move = lift_rows[j]
            at = start + move + b - 1
            zz4[base : base + c0] = row[:, at : at + span]
            row, move = skip_rows[j]
            zz4[base + c0 : base + 2 * c0] = row[:, at : at + span]
    joined = []
    for q in range(2):
        out = dot(w_unite[...], zz4[2 * q * 6 * c0 : (2 * q + 4) * 6 * c0])
        out = gelu(out).astype(BF)
        joined += [out[:c0], out[c0:]]
    rest = quarter - start
    pieces = []
    for k in range(lanes // pitch // 2):
        for m in range(4):
            at = rest + k * pitch + HALO
            pieces.append(joined[m][:, at : at + breadth])
    merged[...] = jnp.concatenate(pieces, axis=1)


def project_kernel(per_section, map_a, map_b, w_out, out, tall):
    section = lax.axis_index("section")
    height, breadth = out.shape[2], out.shape[3]
    for n, source in enumerate((map_a, map_b)):
        full = dot(w_out[...], source[...])
        for i in range(height):
            tall[n, :, i, :] = full[:, i * breadth : (i + 1) * breadth]
        place = section if n == 0 else 1 - section
        out[pl.ds(place, 1)] = tall[n].astype(BF)[None]


def call(kernel, outs, scratch, args, spaces=None):
    vmem = pl.BlockSpec(memory_space=pltpu.VMEM)
    return pl.pallas_call(
        kernel,
        out_shape=outs,
        in_specs=spaces if spaces else [vmem] * len(args),
        out_specs=jax.tree.map(lambda _: vmem, outs),
        scratch_shapes=scratch,
        compiler_params=pltpu.CompilerParams(vmem_limit_bytes=56 << 20),
    )(*args)


def shards(fields_in, plan, in_proj, enc_conv, down_conv, mid_conv, up_proj, unite_conv, out_proj):
    samples, variables, height, breadth = fields_in.shape
    c0, c1 = in_proj.shape[0], up_proj.shape[1]
    sections, lats, lons = lax.axis_size("section"), lax.axis_size("lat"), lax.axis_size("lon")
    shape = jax.ShapeDtypeStruct
    pitch = breadth + 2 * HALO
    lanes = height // 2 * pitch

    def by_row(kernel):
        return kernel.transpose(1, 0, 2).reshape(kernel.shape[1], -1)

    def paired(kernel):
        flat = by_row(kernel)
        third = flat.shape[1] // 3
        return jnp.concatenate([jnp.pad(flat, ((0, 0), (0, third))), jnp.pad(flat, ((0, 0), (third, 0)))], axis=0)

    w_enc, w_unite = paired(enc_conv), paired(unite_conv)
    w_down, w_mid = by_row(down_conv), by_row(mid_conv)

    strip = shape((samples, c0, height * HALO), BF)
    stem, strip_x, strip_y = call(
        stem_kernel,
        (shape((samples, c0, height * breadth), BF), strip, strip),
        [pltpu.VMEM((samples, variables, height, breadth), F32)],
        (fields_in, in_proj),
    )
    recv_x = lax.ppermute(strip_x, "lon", swap_pairs(lons, False, True))
    recv_y = lax.ppermute(strip_y, "lon", swap_pairs(lons, True, True))
    half = shape((samples, c0, lanes), BF)
    half_x, half_y = call(
        lambda *refs: widen_kernel(breadth, *refs), (half, half), [], (stem, recv_x, recv_y)
    )
    far_x = lax.ppermute(half_x, "lat", swap_pairs(lats, False, False))
    far_y = lax.ppermute(half_y, "lat", swap_pairs(lats, True, False))
    hbm, vmem, smem = (pl.BlockSpec(memory_space=s) for s in (pl.ANY, pltpu.VMEM, pltpu.SMEM))
    half_lanes = -(-lanes // 256) * 128
    span = -(-(3 * (lanes // 4)) // 128) * 128 - lanes // 4 // 128 * 128

    def unet(which):
        return call(
            lambda *refs: unet_kernel(which, samples, lats, breadth, *refs),
            shape((c0, height * breadth), BF),
            [
                pltpu.VMEM((4, c0, lanes), BF),
                pltpu.VMEM((6 * 3 * c0, lanes), BF),
                pltpu.VMEM((4 * 3 * c0, half_lanes), BF),
                pltpu.VMEM((4 * 3 * c1, half_lanes), BF),
                pltpu.VMEM((6 * 6 * c0, span), BF),
                pltpu.SemaphoreType.DMA((4,)),
            ],
            (plan, half_x, half_y, far_x, far_y, w_enc, w_down, w_mid, up_proj, w_unite),
            [smem] + [hbm] * 4 + [vmem] * 5,
        )

    across = [(0, 1), (1, 0)]
    map_a = lax.ppermute(unet(0), "section", across)
    map_b = unet(1)
    map_b = lax.cond(
        plan[samples - 1] >= samples, lambda v: lax.ppermute(v, "section", across), lambda v: v, map_b
    )
    return call(
        lambda *refs: project_kernel(samples, *refs),
        shape((samples, variables, height, breadth), BF),
        [pltpu.VMEM((2, variables, height, breadth), F32)],
        (map_a, map_b, out_proj),
    )


def solution(mesh):
    return jax.shard_map(
        shards,
        mesh=mesh,
        in_specs=(P("section", None, "lat", "lon"), P(), P(), P(), P(), P(), P(), P(), P()),
        out_specs=P("section", None, "lat", "lon"),
        check_vma=False,
    )
```

```python
import jax
import jax.numpy as jnp
from jax import lax
from jax.experimental import pallas as pl
from jax.experimental.pallas import tpu as pltpu
from jax.sharding import PartitionSpec as P

BF = jnp.bfloat16
F32 = jnp.float32
HALO = 8


def gelu(x):
    inner = x * (0.7978845608028654 + 0.035677408136300125 * (x * x))
    half = 0.5 * x
    return half + half * jnp.tanh(inner)


def dot(a, b):
    return jnp.dot(a, b, preferred_element_type=F32)


def across(a, b):
    return lax.dot_general(a, b, (((0,), (0,)), ((), ())), preferred_element_type=F32)


def shift(x, by):
    n = x.shape[1]
    by = by % n
    if by == 0:
        return x
    return jnp.concatenate([x[:, by:], x[:, :by]], axis=1)


def swap_pairs(count, odd, periodic):
    pairs = []
    for low in range(1 if odd else 0, count, 2):
        high = low + 1
        if high >= count:
            if not periodic:
                continue
            high = 0
        pairs += [(low, high), (high, low)]
    return pairs


def stem_kernel(fields, w_in, stem, strip_x, strip_y, held, weights, tall, sems):
    samples, variables, height, breadth = fields.shape
    odd = lax.axis_index("lon") % 2
    first = pltpu.make_async_copy(w_in, weights, sems.at[samples])
    first.start()
    loads = [pltpu.make_async_copy(fields.at[b], held.at[b], sems.at[b]) for b in range(samples)]
    for load in loads:
        load.start()
    first.wait()
    for b in range(samples):
        loads[b].wait()
        tall[b] = held[b].astype(F32)
        cols = []
        for i in range(height):
            cols.append(tall[b, :, i, :].astype(BF))
        picked = jnp.concatenate(cols, axis=1)
        full = gelu(dot(weights[...], picked)).astype(BF)
        stem[b] = full
        left = jnp.concatenate([full[:, i * breadth : i * breadth + HALO] for i in range(height)], axis=1)
        right = jnp.concatenate(
            [full[:, (i + 1) * breadth - HALO : (i + 1) * breadth] for i in range(height)], axis=1
        )
        strip_x[b] = jnp.where(odd == 1, left, right)
        strip_y[b] = jnp.where(odd == 1, right, left)


def widen_kernel(breadth, stem, recv_x, recv_y, half_x, half_y):
    samples = stem.shape[0]
    height = stem.shape[2] // breadth
    half = height // 2
    lon_odd = lax.axis_index("lon") % 2
    lat_odd = lax.axis_index("lat") % 2
    for b in range(samples):
        full = stem[b]
        from_x, from_y = recv_x[b], recv_y[b]
        left = jnp.where(lon_odd == 1, from_x, from_y)
        right = jnp.where(lon_odd == 1, from_y, from_x)
        halves = []
        for first in (0, half):
            pieces = []
            for m in range(4):
                for k in range(half // 4):
                    i = first + 4 * k + m
                    pieces += [
                        left[:, i * HALO : (i + 1) * HALO],
                        full[:, i * breadth : (i + 1) * breadth],
                        right[:, i * HALO : (i + 1) * HALO],
                    ]
            halves.append(jnp.concatenate(pieces, axis=1))
        half_x[b] = jnp.where(lat_odd == 1, halves[0], halves[1])
        half_y[b] = jnp.where(lat_odd == 1, halves[1], halves[0])


def by_row(kernel):
    return jnp.concatenate([kernel[n] for n in range(kernel.shape[0])], axis=1)


def paired(kernel):
    flat = by_row(kernel)
    zeros = jnp.zeros((flat.shape[0], flat.shape[1] // 3), BF)
    return jnp.concatenate(
        [jnp.concatenate([flat, zeros], axis=1), jnp.concatenate([zeros, flat], axis=1)], axis=0
    )


def unet_kernel(
    which, per_section, lat_count, breadth, plan, crossing, own_x, own_y, recv_x, recv_y, enc, down, mid, w_up, unite, w_out,
    merged, w_out_held, quads, zz1, zz2, zz3, zz4,
):
    pitch = breadth + 2 * HALO
    lat = lax.axis_index("lat")
    section = lax.axis_index("section")
    odd = lat % 2
    first_turn = plan[0] - per_section
    last_turn = plan[2 * per_section - 1]
    sample = jnp.where(section == 0, last_turn, first_turn)
    if which == 1:
        sample = 1 - sample
    even = odd == 0
    mine_x, mine_y, far_x, far_y = own_x[sample], own_y[sample], recv_x[sample], recv_y[sample]
    quads[0] = jnp.where(even, far_y, far_x)
    quads[1] = jnp.where(even, mine_y, mine_x)
    quads[2] = jnp.where(even, mine_x, mine_y)
    quads[3] = jnp.where(even, far_x, far_y)
    c0 = quads.shape[1]
    lanes = quads.shape[2]
    quarter = lanes // 4
    low_edge = lat == 0
    high_edge = lat == lat_count - 1

    def keep(width, low, high):
        lane = lax.broadcasted_iota(jnp.int32, (1, width), 1)
        drop = (low_edge & (lane < low)) | (high_edge & (lane >= high))
        return jnp.where(drop, 0.0, 1.0).astype(F32)

    full_keep = keep(lanes, quarter, lanes - quarter)
    planes = [
        jnp.concatenate([quads[s, :, m * quarter : (m + 1) * quarter] for s in range(4)], axis=1)
        for m in range(4)
    ]
    rows = [shift(planes[3], -pitch)] + planes + [shift(planes[0], pitch)]
    for j, row in enumerate(rows):
        base = j * 3 * c0
        zz1[base : base + c0] = shift(row, -1)
        zz1[base + c0 : base + 2 * c0] = row
        zz1[base + 2 * c0 : base + 3 * c0] = shift(row, 1)
    skip = []
    for q in range(2):
        out = dot(paired(enc), zz1[2 * q * 3 * c0 : (2 * q + 4) * 3 * c0])
        out = (gelu(out) * full_keep).astype(BF)
        skip += [out[:c0], out[c0:]]

    blocks = -(-lanes // 256)
    spare = blocks * 256 - lanes
    to_lane = lax.broadcasted_iota(jnp.int32, (512, 128), 1)
    from_lane = lax.broadcasted_iota(jnp.int32, (512, 128), 0) % 256
    gather = jnp.where(from_lane // 2 == to_lane, 0.25, 0.0).astype(BF)
    stacked = []
    for h in range(2):
        pair = [
            jnp.concatenate([skip[2 * h + e], jnp.zeros((c0, spare), BF)], axis=1) if spare else skip[2 * h + e]
            for e in range(2)
        ]
        for t in range(blocks):
            stacked.append(
                jnp.concatenate([pair[0][:, 256 * t : 256 * (t + 1)], pair[1][:, 256 * t : 256 * (t + 1)]], axis=1)
            )
    small = dot(jnp.concatenate(stacked, axis=0), gather).astype(BF)
    pooled = [
        jnp.concatenate([small[(h * blocks + t) * c0 : (h * blocks + t + 1) * c0] for t in range(blocks)], axis=1)
        for h in range(2)
    ]
    half_lanes = 128 * blocks
    half_pitch = pitch // 2
    half_keep = keep(half_lanes, quarter // 2, (lanes - quarter) // 2)

    def halves(scratch, source):
        width = source[0].shape[0]
        for j, row in enumerate(
            (shift(source[1], -half_pitch), source[0], source[1], shift(source[0], half_pitch))
        ):
            base = j * 3 * width
            scratch[base : base + width] = shift(row, -1)
            scratch[base + width : base + 2 * width] = row
            scratch[base + 2 * width : base + 3 * width] = shift(row, 1)

    halves(zz2, pooled)
    w_down = jnp.concatenate([down[n] for n in range(down.shape[0])], axis=0)
    deep = []
    for h in range(2):
        out = across(w_down, zz2[h * 3 * c0 : (h + 3) * 3 * c0])
        deep.append((gelu(out) * half_keep).astype(BF))
    halves(zz3, deep)
    c1 = deep[0].shape[0]
    lifted = []
    for h in range(2):
        out = dot(by_row(mid), zz3[h * 3 * c1 : (h + 3) * 3 * c1])
        middle = (gelu(out) + deep[h].astype(F32)).astype(BF)
        lifted.append((dot(w_up[...], middle) * half_keep).astype(BF))
    wide_lane = lax.broadcasted_iota(jnp.int32, (128, 256), 1)
    thin_lane = lax.broadcasted_iota(jnp.int32, (128, 256), 0)
    spread = jnp.where(wide_lane // 2 == thin_lane, 1.0, 0.0).astype(BF)
    stacked = jnp.concatenate(
        [lifted[h][:, 128 * t : 128 * (t + 1)] for h in range(2) for t in range(blocks)], axis=0
    )
    large = dot(stacked, spread).astype(BF)
    raised = [
        jnp.concatenate([large[(h * blocks + t) * c0 : (h * blocks + t + 1) * c0] for t in range(blocks)], axis=1)
        for h in range(2)
    ]
    start = quarter // 128 * 128
    span = zz4.shape[1]
    lift_rows = [(raised[1], -pitch), (raised[0], 0), (raised[0], 0), (raised[1], 0), (raised[1], 0), (raised[0], pitch)]
    skip_rows = [(skip[3], -pitch)] + [(s, 0) for s in skip] + [(skip[0], pitch)]
    for j in range(6):
        for b in range(3):
            base = (3 * j + b) * 2 * c0
            row, move = lift_rows[j]
            at = start + move + b - 1
            zz4[base : base + c0] = row[:, at : at + span]
            row, move = skip_rows[j]
            zz4[base + c0 : base + 2 * c0] = row[:, at : at + span]
    joined = []
    for q in range(2):
        out = dot(paired(unite), zz4[2 * q * 6 * c0 : (2 * q + 4) * 6 * c0])
        out = gelu(out).astype(BF)
        joined += [out[:c0], out[c0:]]
    rest = quarter - start
    pieces = []
    for k in range(lanes // pitch // 2):
        for m in range(4):
            at = rest + k * pitch + HALO
            pieces.append(joined[m][:, at : at + breadth])
    merged[...] = jnp.concatenate(pieces, axis=1)
    w_out_held[...] = w_out[...]


def project_kernel(map_a, map_b, w_out, out, tall, ready, sems):
    section = lax.axis_index("section")
    height, breadth = out.shape[2], out.shape[3]
    stores = []
    for n, source in enumerate((map_b, map_a)):
        full = across(w_out[...], source[...])
        for i in range(height):
            tall[n, :, i, :] = full[:, i * breadth : (i + 1) * breadth]
        ready[n] = tall[n].astype(BF)
        store = pltpu.make_async_copy(ready.at[n], out.at[section if n == 1 else 1 - section], sems.at[n])
        store.start()
        stores.append(store)
    for store in stores:
        store.wait()


def call(kernel, outs, scratch, args, mebibytes, spaces=None, out_space=None):
    vmem = pl.BlockSpec(memory_space=pltpu.VMEM)
    return pl.pallas_call(
        kernel,
        out_shape=outs,
        in_specs=spaces if spaces else [vmem] * len(args),
        out_specs=jax.tree.map(lambda _: out_space or vmem, outs),
        scratch_shapes=scratch,
        compiler_params=pltpu.CompilerParams(vmem_limit_bytes=mebibytes << 20),
    )(*args)


def shards(fields_in, plan, in_proj, enc_conv, down_conv, mid_conv, up_proj, unite_conv, out_proj):
    samples, variables, height, breadth = fields_in.shape
    c0, c1 = in_proj.shape[0], up_proj.shape[1]
    sections, lats, lons = lax.axis_size("section"), lax.axis_size("lat"), lax.axis_size("lon")
    shape = jax.ShapeDtypeStruct
    lanes = height // 2 * (breadth + 2 * HALO)

    hbm, vmem, smem = (pl.BlockSpec(memory_space=s) for s in (pl.ANY, pltpu.VMEM, pltpu.SMEM))
    crossing = (plan[samples - 1] >= samples).astype(jnp.int32)
    strip = shape((samples, c0, height * HALO), BF)
    stem, strip_x, strip_y = call(
        stem_kernel,
        (shape((samples, c0, height * breadth), BF), strip, strip),
        [
            pltpu.VMEM((samples, variables, height, breadth), BF),
            pltpu.VMEM((c0, variables), BF),
            pltpu.VMEM((samples, variables, height, breadth), F32),
            pltpu.SemaphoreType.DMA((samples + 1,)),
        ],
        (fields_in, in_proj),
        12,
        [hbm, hbm],
    )
    recv_y = lax.ppermute(strip_y, "lon", swap_pairs(lons, True, True))
    recv_x = lax.ppermute(strip_x, "lon", swap_pairs(lons, False, True))
    half = shape((samples, c0, lanes), BF)
    half_x, half_y = call(
        lambda *refs: widen_kernel(breadth, *refs), (half, half), [], (stem, recv_x, recv_y), 8
    )
    far_y = lax.ppermute(half_y, "lat", swap_pairs(lats, True, False))
    far_x = lax.ppermute(half_x, "lat", swap_pairs(lats, False, False))
    half_lanes = -(-lanes // 256) * 128
    span = -(-(3 * (lanes // 4)) // 128) * 128 - lanes // 4 // 128 * 128

    def unet(which):
        return call(
            lambda *refs: unet_kernel(which, samples, lats, breadth, *refs),
            (shape((c0, height * breadth), BF), shape((c0, variables), BF)),
            [
                pltpu.VMEM((4, c0, lanes), BF),
                pltpu.VMEM((6 * 3 * c0, lanes), BF),
                pltpu.VMEM((4 * 3 * c0, half_lanes), BF),
                pltpu.VMEM((4 * 3 * c1, half_lanes), BF),
                pltpu.VMEM((6 * 6 * c0, span), BF),
            ],
            (plan, crossing[None], half_x, half_y, far_x, far_y, enc_conv, down_conv.transpose(0, 2, 1), mid_conv)
            + (up_proj, unite_conv, out_proj.T),
            20,
            [smem] * 2 + [vmem] * 10,
        )

    swap = [(0, 1), (1, 0)]
    map_a = lax.ppermute(unet(0)[0], "section", swap)
    map_b, w_out = unet(1)
    map_b = lax.cond(
        crossing > 0, lambda v: lax.ppermute(v, "section", swap), lambda v: v, map_b
    )
    return call(
        project_kernel,
        shape((samples, variables, height, breadth), BF),
        [
            pltpu.VMEM((2, variables, height, breadth), F32),
            pltpu.VMEM((2, variables, height, breadth), BF),
            pltpu.SemaphoreType.DMA((2,)),
        ],
        (map_a, map_b, w_out),
        12,
        out_space=hbm,
    )


def solution(mesh):
    return jax.shard_map(
        shards,
        mesh=mesh,
        in_specs=(P("section", None, "lat", "lon"), P(), P(), P(), P(), P(), P(), P(), P()),
        out_specs=P("section", None, "lat", "lon"),
        check_vma=False,
    )
```

```python
import jax
import jax.numpy as jnp
from jax import lax
from jax.experimental import pallas as pl
from jax.experimental.pallas import tpu as pltpu
from jax.sharding import PartitionSpec as P

BF = jnp.bfloat16
F32 = jnp.float32
HALO = 8


def gelu(x):
    inner = x * (0.7978845608028654 + 0.035677408136300125 * (x * x))
    half = 0.5 * x
    return half + half * jnp.tanh(inner)


def dot(a, b):
    return jnp.dot(a, b, preferred_element_type=F32)


def across(a, b):
    return lax.dot_general(a, b, (((0,), (0,)), ((), ())), preferred_element_type=F32)


def shift(x, by):
    n = x.shape[1]
    by = by % n
    if by == 0:
        return x
    return jnp.concatenate([x[:, by:], x[:, :by]], axis=1)


def swap_pairs(count, odd, periodic):
    pairs = []
    for low in range(1 if odd else 0, count, 2):
        high = low + 1
        if high >= count:
            if not periodic:
                continue
            high = 0
        pairs += [(low, high), (high, low)]
    return pairs


def stem_kernel(fields, w_in, stem, strip_x, strip_y, held, weights, tall, sems):
    samples, variables, height, breadth = fields.shape
    odd = lax.axis_index("lon") % 2
    first = pltpu.make_async_copy(w_in, weights, sems.at[samples])
    first.start()
    loads = [pltpu.make_async_copy(fields.at[b], held.at[b], sems.at[b]) for b in range(samples)]
    for load in loads:
        load.start()
    first.wait()
    for b in range(samples):
        loads[b].wait()
        tall[...] = held[b].astype(F32).reshape(variables * height, breadth)
        cols = [tall[pl.ds(i, variables, stride=height), :].astype(BF) for i in range(height)]
        picked = jnp.concatenate(cols, axis=1)
        full = gelu(dot(weights[...], picked)).astype(BF)
        stem[b] = full
        left = jnp.concatenate([full[:, i * breadth : i * breadth + HALO] for i in range(height)], axis=1)
        right = jnp.concatenate(
            [full[:, (i + 1) * breadth - HALO : (i + 1) * breadth] for i in range(height)], axis=1
        )
        strip_x[b] = jnp.where(odd == 1, left, right)
        strip_y[b] = jnp.where(odd == 1, right, left)


def widen_kernel(breadth, order, stem, recv_x, recv_y, half_x, half_y):
    samples = stem.shape[0]
    leaving = jnp.max(order[...])
    height = stem.shape[2] // breadth
    half = height // 2
    lon_odd = lax.axis_index("lon") % 2
    lat_odd = lax.axis_index("lat") % 2
    for b in range(samples):
        full = stem[b]
        from_x, from_y = recv_x[b], recv_y[b]
        left = jnp.where(lon_odd == 1, from_x, from_y)
        right = jnp.where(lon_odd == 1, from_y, from_x)
        halves = []
        for first in (0, half):
            pieces = []
            for m in range(4):
                for k in range(half // 4):
                    i = first + 4 * k + m
                    pieces += [
                        left[:, i * HALO : (i + 1) * HALO],
                        full[:, i * breadth : (i + 1) * breadth],
                        right[:, i * HALO : (i + 1) * HALO],
                    ]
            halves.append(jnp.concatenate(pieces, axis=1))
        slot = jnp.where(leaving == b, 0, 1)
        half_x[pl.ds(slot, 1)] = jnp.where(lat_odd == 1, halves[0], halves[1])[None]
        half_y[pl.ds(slot, 1)] = jnp.where(lat_odd == 1, halves[1], halves[0])[None]


def by_row(kernel):
    return jnp.concatenate([kernel[n] for n in range(kernel.shape[0])], axis=1)


def paired(kernel):
    flat = by_row(kernel)
    zeros = jnp.zeros((flat.shape[0], flat.shape[1] // 3), BF)
    return jnp.concatenate(
        [jnp.concatenate([flat, zeros], axis=1), jnp.concatenate([zeros, flat], axis=1)], axis=0
    )


def unet_kernel(which, lat_count, breadth, own_x, own_y, recv_x, recv_y, enc, down, mid, w_up, unite, *refs):
    if which == 1:
        w_out, merged, w_out_held = refs[:3]
        w_out_held[...] = w_out[...]
    else:
        merged = refs[0]
    quads, zz1, zz2, zz3, zz4 = refs[1 + 2 * which :]
    pitch = breadth + 2 * HALO
    lat = lax.axis_index("lat")
    even = lat % 2 == 0
    mine_x, mine_y, far_x, far_y = own_x[which], own_y[which], recv_x[which], recv_y[which]
    quads[0] = jnp.where(even, far_y, far_x)
    quads[1] = jnp.where(even, mine_y, mine_x)
    quads[2] = jnp.where(even, mine_x, mine_y)
    quads[3] = jnp.where(even, far_x, far_y)
    c0 = quads.shape[1]
    lanes = quads.shape[2]
    quarter = lanes // 4
    low_edge = lat == 0
    high_edge = lat == lat_count - 1

    def keep(width, low, high):
        lane = lax.broadcasted_iota(jnp.int32, (1, width), 1)
        drop = (low_edge & (lane < low)) | (high_edge & (lane >= high))
        return jnp.where(drop, 0.0, 1.0).astype(F32)

    full_keep = keep(lanes, quarter, lanes - quarter)
    planes = [
        jnp.concatenate([quads[s, :, m * quarter : (m + 1) * quarter] for s in range(4)], axis=1)
        for m in range(4)
    ]
    rows = [shift(planes[3], -pitch)] + planes + [shift(planes[0], pitch)]
    for j, row in enumerate(rows):
        base = j * 3 * c0
        zz1[base : base + c0] = shift(row, -1)
        zz1[base + c0 : base + 2 * c0] = row
        zz1[base + 2 * c0 : base + 3 * c0] = shift(row, 1)
    skip = []
    for q in range(2):
        out = dot(paired(enc), zz1[2 * q * 3 * c0 : (2 * q + 4) * 3 * c0])
        out = (gelu(out) * full_keep).astype(BF)
        skip += [out[:c0], out[c0:]]

    blocks = -(-lanes // 256)
    spare = blocks * 256 - lanes
    to_lane = lax.broadcasted_iota(jnp.int32, (512, 128), 1)
    from_lane = lax.broadcasted_iota(jnp.int32, (512, 128), 0) % 256
    gather = jnp.where(from_lane // 2 == to_lane, 0.25, 0.0).astype(BF)
    stacked = []
    for h in range(2):
        pair = [
            jnp.concatenate([skip[2 * h + e], jnp.zeros((c0, spare), BF)], axis=1) if spare else skip[2 * h + e]
            for e in range(2)
        ]
        for t in range(blocks):
            stacked.append(
                jnp.concatenate([pair[0][:, 256 * t : 256 * (t + 1)], pair[1][:, 256 * t : 256 * (t + 1)]], axis=1)
            )
    small = dot(jnp.concatenate(stacked, axis=0), gather).astype(BF)
    pooled = [
        jnp.concatenate([small[(h * blocks + t) * c0 : (h * blocks + t + 1) * c0] for t in range(blocks)], axis=1)
        for h in range(2)
    ]
    half_lanes = 128 * blocks
    half_pitch = pitch // 2
    half_keep = keep(half_lanes, quarter // 2, (lanes - quarter) // 2)

    def halves(scratch, source):
        width = source[0].shape[0]
        for j, row in enumerate(
            (shift(source[1], -half_pitch), source[0], source[1], shift(source[0], half_pitch))
        ):
            base = j * 3 * width
            scratch[base : base + width] = shift(row, -1)
            scratch[base + width : base + 2 * width] = row
            scratch[base + 2 * width : base + 3 * width] = shift(row, 1)

    halves(zz2, pooled)
    w_down = jnp.concatenate([down[n] for n in range(down.shape[0])], axis=0)
    deep = []
    for h in range(2):
        out = across(w_down, zz2[h * 3 * c0 : (h + 3) * 3 * c0])
        deep.append((gelu(out) * half_keep).astype(BF))
    halves(zz3, deep)
    c1 = deep[0].shape[0]
    lifted = []
    for h in range(2):
        out = dot(by_row(mid), zz3[h * 3 * c1 : (h + 3) * 3 * c1])
        middle = (gelu(out) + deep[h].astype(F32)).astype(BF)
        lifted.append((dot(w_up[...], middle) * half_keep).astype(BF))
    wide_lane = lax.broadcasted_iota(jnp.int32, (128, 256), 1)
    thin_lane = lax.broadcasted_iota(jnp.int32, (128, 256), 0)
    spread = jnp.where(wide_lane // 2 == thin_lane, 1.0, 0.0).astype(BF)
    stacked = jnp.concatenate(
        [lifted[h][:, 128 * t : 128 * (t + 1)] for h in range(2) for t in range(blocks)], axis=0
    )
    large = dot(stacked, spread).astype(BF)
    raised = [
        jnp.concatenate([large[(h * blocks + t) * c0 : (h * blocks + t + 1) * c0] for t in range(blocks)], axis=1)
        for h in range(2)
    ]
    start = quarter // 128 * 128
    span = zz4.shape[1]
    lift_rows = [(raised[1], -pitch), (raised[0], 0), (raised[0], 0), (raised[1], 0), (raised[1], 0), (raised[0], pitch)]
    skip_rows = [(skip[3], -pitch)] + [(s, 0) for s in skip] + [(skip[0], pitch)]
    for j in range(6):
        for b in range(3):
            base = (3 * j + b) * 2 * c0
            row, move = lift_rows[j]
            at = start + move + b - 1
            zz4[base : base + c0] = row[:, at : at + span]
            row, move = skip_rows[j]
            zz4[base + c0 : base + 2 * c0] = row[:, at : at + span]
    joined = []
    for q in range(2):
        out = dot(paired(unite), zz4[2 * q * 6 * c0 : (2 * q + 4) * 6 * c0])
        out = gelu(out).astype(BF)
        joined += [out[:c0], out[c0:]]
    rest = quarter - start
    pieces = []
    for k in range(lanes // pitch // 2):
        for m in range(4):
            at = rest + k * pitch + HALO
            pieces.append(joined[m][:, at : at + breadth])
    merged[...] = jnp.concatenate(pieces, axis=1)


def project_kernel(map_a, map_b, w_out, out, tall, ready, sems):
    section = lax.axis_index("section")
    variables, height, breadth = out.shape[1:]
    stores = []
    for n, source in enumerate((map_b, map_a)):
        full = across(w_out[...], source[...])
        for i in range(height):
            tall[n, pl.ds(i, variables, stride=height), :] = full[:, i * breadth : (i + 1) * breadth]
        ready[n] = tall[n].astype(BF).reshape(variables, height, breadth)
        store = pltpu.make_async_copy(ready.at[n], out.at[section if n == 1 else 1 - section], sems.at[n])
        store.start()
        stores.append(store)
    for store in stores:
        store.wait()


def call(kernel, outs, scratch, args, mebibytes, spaces=None, out_space=None):
    vmem = pl.BlockSpec(memory_space=pltpu.VMEM)
    return pl.pallas_call(
        kernel,
        out_shape=outs,
        in_specs=spaces if spaces else [vmem] * len(args),
        out_specs=out_space or jax.tree.map(lambda _: vmem, outs),
        scratch_shapes=scratch,
        compiler_params=pltpu.CompilerParams(vmem_limit_bytes=int(mebibytes * 2**20)),
    )(*args)


def shards(fields_in, plan, in_proj, enc_conv, down_conv, mid_conv, up_proj, unite_conv, out_proj):
    samples, variables, height, breadth = fields_in.shape
    c0, c1 = in_proj.shape[0], up_proj.shape[1]
    sections, lats, lons = lax.axis_size("section"), lax.axis_size("lat"), lax.axis_size("lon")
    shape = jax.ShapeDtypeStruct
    lanes = height // 2 * (breadth + 2 * HALO)

    hbm, vmem, smem = (pl.BlockSpec(memory_space=s) for s in (pltpu.HBM, pltpu.VMEM, pltpu.SMEM))
    strip = shape((samples, c0, height * HALO), BF)
    stem, strip_x, strip_y = call(
        stem_kernel,
        (shape((samples, c0, height * breadth), BF), strip, strip),
        [
            pltpu.VMEM((samples, variables, height, breadth), BF),
            pltpu.VMEM((c0, variables), BF),
            pltpu.VMEM((variables * height, breadth), F32),
            pltpu.SemaphoreType.DMA((samples + 1,)),
        ],
        (fields_in, in_proj),
        53,
        [hbm, hbm],
    )
    recv_y = lax.ppermute(strip_y, "lon", swap_pairs(lons, True, True))
    recv_x = lax.ppermute(strip_x, "lon", swap_pairs(lons, False, True))
    half = shape((samples, c0, lanes), BF)
    leaving = jnp.where(lax.axis_index("section") == 0, plan[2 * samples - 1], plan[0] - samples)
    order = jnp.broadcast_to(leaving.astype(F32), (8, 128))
    crossing = (plan[samples - 1] >= samples).astype(jnp.int32)
    recv_x, recv_y, order, crossing = lax.optimization_barrier((recv_x, recv_y, order, crossing))
    half_x, half_y = call(
        lambda *refs: widen_kernel(breadth, *refs), (half, half), [], (order, stem, recv_x, recv_y), 8
    )
    far_y = lax.ppermute(half_y, "lat", swap_pairs(lats, True, False))
    far_x = lax.ppermute(half_x, "lat", swap_pairs(lats, False, False))
    half_lanes = -(-lanes // 256) * 128
    span = -(-(3 * (lanes // 4)) // 128) * 128 - lanes // 4 // 128 * 128

    def unet(which):
        return call(
            lambda *refs: unet_kernel(which, lats, breadth, *refs),
            (shape((c0, height * breadth), BF), shape((c0, variables), BF))[: 1 + which],
            [
                pltpu.VMEM((4, c0, lanes), BF),
                pltpu.VMEM((6 * 3 * c0, lanes), BF),
                pltpu.VMEM((4 * 3 * c0, half_lanes), BF),
                pltpu.VMEM((4 * 3 * c1, half_lanes), BF),
                pltpu.VMEM((6 * 6 * c0, span), BF),
            ],
            (half_x, half_y, far_x, far_y, enc_conv, down_conv.transpose(0, 2, 1), mid_conv)
            + (up_proj, unite_conv, out_proj.T)[: 2 + which],
            20,
            [vmem] * (9 + which),
        )

    swap = [(0, 1), (1, 0)]
    map_a = lax.ppermute(unet(0)[0], "section", swap)
    map_b, w_out = unet(1)
    map_b = lax.cond(
        crossing > 0, lambda v: lax.ppermute(v, "section", swap), lambda v: v, map_b
    )
    return call(
        project_kernel,
        shape((samples, variables, height, breadth), BF),
        [
            pltpu.VMEM((2, variables * height, breadth), F32),
            pltpu.VMEM((2, variables, height, breadth), BF),
            pltpu.SemaphoreType.DMA((2,)),
        ],
        (map_a, map_b, w_out),
        12,
        out_space=hbm,
    )


def solution(mesh):
    return jax.shard_map(
        shards,
        mesh=mesh,
        in_specs=(P("section", None, "lat", "lon"), P(), P(), P(), P(), P(), P(), P(), P()),
        out_specs=P("section", None, "lat", "lon"),
        check_vma=False,
    )
```

```python
import jax
import jax.numpy as jnp
from jax import lax
from jax.experimental import pallas as pl
from jax.experimental.pallas import tpu as pltpu
from jax.sharding import PartitionSpec as P

BF = jnp.bfloat16
F32 = jnp.float32
HALO = 8
LIMIT_ROWS = 52.7


def gelu(x):
    inner = x * (0.7978845608028654 + 0.035677408136300125 * (x * x))
    half = 0.5 * x
    return half + half * jnp.tanh(inner)


def dot(a, b):
    return jnp.dot(a, b, preferred_element_type=F32)


def across(a, b):
    return lax.dot_general(a, b, (((0,), (0,)), ((), ())), preferred_element_type=F32)


def shift(x, by):
    n = x.shape[1]
    by = by % n
    if by == 0:
        return x
    return jnp.concatenate([x[:, by:], x[:, :by]], axis=1)


def swap_pairs(count, odd, periodic):
    pairs = []
    for low in range(1 if odd else 0, count, 2):
        high = low + 1
        if high >= count:
            if not periodic:
                continue
            high = 0
        pairs += [(low, high), (high, low)]
    return pairs


def rows_kernel(fields, picked, held, tall, sems):
    samples, variables, height, breadth = fields.shape
    loads = [pltpu.make_async_copy(fields.at[b], held.at[b], sems.at[b]) for b in range(samples)]
    for load in loads:
        load.start()
    for b in range(samples):
        loads[b].wait()
        tall[...] = held[b].astype(F32).reshape(variables * height, breadth)
        for i in range(height):
            picked[b, :, i * breadth : (i + 1) * breadth] = tall[pl.ds(i, variables, stride=height), :].astype(BF)


def stem_kernel(height, breadth, picked, w_in, stem, strip_x, strip_y):
    samples = picked.shape[0]
    odd = lax.axis_index("lon") % 2
    for b in range(samples):
        full = gelu(dot(w_in[...], picked[b])).astype(BF)
        stem[b] = full
        left = jnp.concatenate([full[:, i * breadth : i * breadth + HALO] for i in range(height)], axis=1)
        right = jnp.concatenate(
            [full[:, (i + 1) * breadth - HALO : (i + 1) * breadth] for i in range(height)], axis=1
        )
        strip_x[b] = jnp.where(odd == 1, left, right)
        strip_y[b] = jnp.where(odd == 1, right, left)


def widen_kernel(breadth, plan, stem, recv_x, recv_y, half_x, half_y):
    samples = stem.shape[0]
    turns = plan[...].astype(F32).reshape(1, 2 * samples)
    turn = lax.broadcasted_iota(jnp.int32, turns.shape, 1)
    first, last = (jnp.sum(jnp.where(turn == n, turns, 0.0)) for n in (0, 2 * samples - 1))
    leaving = jnp.where(lax.axis_index("section") == 0, last, first - samples)
    height = stem.shape[2] // breadth
    half = height // 2
    lon_odd = lax.axis_index("lon") % 2
    lat_odd = lax.axis_index("lat") % 2
    for b in range(samples):
        full = stem[b]
        from_x, from_y = recv_x[b], recv_y[b]
        left = jnp.where(lon_odd == 1, from_x, from_y)
        right = jnp.where(lon_odd == 1, from_y, from_x)
        halves = []
        for first in (0, half):
            pieces = []
            for m in range(4):
                for k in range(half // 4):
                    i = first + 4 * k + m
                    pieces += [
                        left[:, i * HALO : (i + 1) * HALO],
                        full[:, i * breadth : (i + 1) * breadth],
                        right[:, i * HALO : (i + 1) * HALO],
                    ]
            halves.append(jnp.concatenate(pieces, axis=1))
        slot = jnp.where(leaving == b, 0, 1)
        half_x[pl.ds(slot, 1)] = jnp.where(lat_odd == 1, halves[0], halves[1])[None]
        half_y[pl.ds(slot, 1)] = jnp.where(lat_odd == 1, halves[1], halves[0])[None]


def by_row(kernel):
    return jnp.concatenate([kernel[n] for n in range(kernel.shape[0])], axis=1)


def paired(kernel):
    flat = by_row(kernel)
    zeros = jnp.zeros((flat.shape[0], flat.shape[1] // 3), BF)
    return jnp.concatenate(
        [jnp.concatenate([flat, zeros], axis=1), jnp.concatenate([zeros, flat], axis=1)], axis=0
    )


def unet_kernel(which, lat_count, breadth, own_x, own_y, recv_x, recv_y, enc, down, mid, w_up, unite, *refs):
    if which == 1:
        w_out, merged, w_out_held = refs[:3]
        w_out_held[...] = w_out[...]
    else:
        merged = refs[0]
    quads, zz1, zz2, zz3, zz4 = refs[1 + 2 * which :]
    pitch = breadth + 2 * HALO
    lat = lax.axis_index("lat")
    even = lat % 2 == 0
    mine_x, mine_y, far_x, far_y = own_x[which], own_y[which], recv_x[which], recv_y[which]
    quads[0] = jnp.where(even, far_y, far_x)
    quads[1] = jnp.where(even, mine_y, mine_x)
    quads[2] = jnp.where(even, mine_x, mine_y)
    quads[3] = jnp.where(even, far_x, far_y)
    c0 = quads.shape[1]
    lanes = quads.shape[2]
    quarter = lanes // 4
    low_edge = lat == 0
    high_edge = lat == lat_count - 1

    def keep(width, low, high):
        lane = lax.broadcasted_iota(jnp.int32, (1, width), 1)
        drop = (low_edge & (lane < low)) | (high_edge & (lane >= high))
        return jnp.where(drop, 0.0, 1.0).astype(F32)

    full_keep = keep(lanes, quarter, lanes - quarter)
    planes = [
        jnp.concatenate([quads[s, :, m * quarter : (m + 1) * quarter] for s in range(4)], axis=1)
        for m in range(4)
    ]
    rows = [shift(planes[3], -pitch)] + planes + [shift(planes[0], pitch)]
    for j, row in enumerate(rows):
        base = j * 3 * c0
        zz1[base : base + c0] = shift(row, -1)
        zz1[base + c0 : base + 2 * c0] = row
        zz1[base + 2 * c0 : base + 3 * c0] = shift(row, 1)
    skip = []
    for q in range(2):
        out = dot(paired(enc), zz1[2 * q * 3 * c0 : (2 * q + 4) * 3 * c0])
        out = (gelu(out) * full_keep).astype(BF)
        skip += [out[:c0], out[c0:]]

    blocks = -(-lanes // 256)
    spare = blocks * 256 - lanes
    to_lane = lax.broadcasted_iota(jnp.int32, (512, 128), 1)
    from_lane = lax.broadcasted_iota(jnp.int32, (512, 128), 0) % 256
    gather = jnp.where(from_lane // 2 == to_lane, 0.25, 0.0).astype(BF)
    stacked = []
    for h in range(2):
        pair = [
            jnp.concatenate([skip[2 * h + e], jnp.zeros((c0, spare), BF)], axis=1) if spare else skip[2 * h + e]
            for e in range(2)
        ]
        for t in range(blocks):
            stacked.append(
                jnp.concatenate([pair[0][:, 256 * t : 256 * (t + 1)], pair[1][:, 256 * t : 256 * (t + 1)]], axis=1)
            )
    small = dot(jnp.concatenate(stacked, axis=0), gather).astype(BF)
    pooled = [
        jnp.concatenate([small[(h * blocks + t) * c0 : (h * blocks + t + 1) * c0] for t in range(blocks)], axis=1)
        for h in range(2)
    ]
    half_lanes = 128 * blocks
    half_pitch = pitch // 2
    half_keep = keep(half_lanes, quarter // 2, (lanes - quarter) // 2)

    def halves(scratch, source):
        width = source[0].shape[0]
        for j, row in enumerate(
            (shift(source[1], -half_pitch), source[0], source[1], shift(source[0], half_pitch))
        ):
            base = j * 3 * width
            scratch[base : base + width] = shift(row, -1)
            scratch[base + width : base + 2 * width] = row
            scratch[base + 2 * width : base + 3 * width] = shift(row, 1)

    halves(zz2, pooled)
    w_down = jnp.concatenate([down[n] for n in range(down.shape[0])], axis=0)
    deep = []
    for h in range(2):
        out = across(w_down, zz2[h * 3 * c0 : (h + 3) * 3 * c0])
        deep.append((gelu(out) * half_keep).astype(BF))
    halves(zz3, deep)
    c1 = deep[0].shape[0]
    lifted = []
    for h in range(2):
        out = dot(by_row(mid), zz3[h * 3 * c1 : (h + 3) * 3 * c1])
        middle = (gelu(out) + deep[h].astype(F32)).astype(BF)
        lifted.append((dot(w_up[...], middle) * half_keep).astype(BF))
    wide_lane = lax.broadcasted_iota(jnp.int32, (128, 256), 1)
    thin_lane = lax.broadcasted_iota(jnp.int32, (128, 256), 0)
    spread = jnp.where(wide_lane // 2 == thin_lane, 1.0, 0.0).astype(BF)
    stacked = jnp.concatenate(
        [lifted[h][:, 128 * t : 128 * (t + 1)] for h in range(2) for t in range(blocks)], axis=0
    )
    large = dot(stacked, spread).astype(BF)
    raised = [
        jnp.concatenate([large[(h * blocks + t) * c0 : (h * blocks + t + 1) * c0] for t in range(blocks)], axis=1)
        for h in range(2)
    ]
    start = quarter // 128 * 128
    span = zz4.shape[1]
    lift_rows = [(raised[1], -pitch), (raised[0], 0), (raised[0], 0), (raised[1], 0), (raised[1], 0), (raised[0], pitch)]
    skip_rows = [(skip[3], -pitch)] + [(s, 0) for s in skip] + [(skip[0], pitch)]
    for j in range(6):
        for b in range(3):
            base = (3 * j + b) * 2 * c0
            row, move = lift_rows[j]
            at = start + move + b - 1
            zz4[base : base + c0] = row[:, at : at + span]
            row, move = skip_rows[j]
            zz4[base + c0 : base + 2 * c0] = row[:, at : at + span]
    joined = []
    for q in range(2):
        out = dot(paired(unite), zz4[2 * q * 6 * c0 : (2 * q + 4) * 6 * c0])
        out = gelu(out).astype(BF)
        joined += [out[:c0], out[c0:]]
    rest = quarter - start
    pieces = []
    for k in range(lanes // pitch // 2):
        for m in range(4):
            at = rest + k * pitch + HALO
            pieces.append(joined[m][:, at : at + breadth])
    merged[...] = jnp.concatenate(pieces, axis=1)


def project_kernel(map_a, map_b, w_out, out, tall, ready, sems):
    section = lax.axis_index("section")
    variables, height, breadth = out.shape[1:]
    stores = []
    for n, source in enumerate((map_b, map_a)):
        full = across(w_out[...], source[...])
        for i in range(height):
            tall[n, pl.ds(i, variables, stride=height), :] = full[:, i * breadth : (i + 1) * breadth]
        ready[n] = tall[n].astype(BF).reshape(variables, height, breadth)
        store = pltpu.make_async_copy(ready.at[n], out.at[section if n == 1 else 1 - section], sems.at[n])
        store.start()
        stores.append(store)
    for store in stores:
        store.wait()


def call(kernel, outs, scratch, args, mebibytes, spaces=None, out_space=None):
    vmem = pl.BlockSpec(memory_space=pltpu.VMEM)
    return pl.pallas_call(
        kernel,
        out_shape=outs,
        in_specs=spaces if spaces else [vmem] * len(args),
        out_specs=out_space or jax.tree.map(lambda _: vmem, outs),
        scratch_shapes=scratch,
        compiler_params=pltpu.CompilerParams(vmem_limit_bytes=int(mebibytes * 2**20)),
    )(*args)


def shards(fields_in, plan, in_proj, enc_conv, down_conv, mid_conv, up_proj, unite_conv, out_proj):
    samples, variables, height, breadth = fields_in.shape
    c0, c1 = in_proj.shape[0], up_proj.shape[1]
    sections, lats, lons = lax.axis_size("section"), lax.axis_size("lat"), lax.axis_size("lon")
    shape = jax.ShapeDtypeStruct
    lanes = height // 2 * (breadth + 2 * HALO)

    hbm, vmem, smem = (pl.BlockSpec(memory_space=s) for s in (pltpu.HBM, pltpu.VMEM, pltpu.SMEM))
    strip = shape((samples, c0, height * HALO), BF)
    picked = call(
        rows_kernel,
        shape((samples, variables, height * breadth), BF),
        [
            pltpu.VMEM((samples, variables, height, breadth), BF),
            pltpu.VMEM((variables * height, breadth), F32),
            pltpu.SemaphoreType.DMA((samples,)),
        ],
        (fields_in,),
        LIMIT_ROWS,
        [hbm],
    )
    stem, strip_x, strip_y = call(
        lambda *refs: stem_kernel(height, breadth, *refs),
        (shape((samples, c0, height * breadth), BF), strip, strip),
        [],
        (picked, in_proj),
        12,
    )
    recv_y = lax.ppermute(strip_y, "lon", swap_pairs(lons, True, True))
    recv_x = lax.ppermute(strip_x, "lon", swap_pairs(lons, False, True))
    half = shape((samples, c0, lanes), BF)
    crossing = (plan[samples - 1] >= samples).astype(jnp.int32)
    recv_x, recv_y, crossing = lax.optimization_barrier((recv_x, recv_y, crossing))
    half_x, half_y = call(
        lambda *refs: widen_kernel(breadth, *refs), (half, half), [], (plan, stem, recv_x, recv_y), 8
    )
    far_y = lax.ppermute(half_y, "lat", swap_pairs(lats, True, False))
    far_x = lax.ppermute(half_x, "lat", swap_pairs(lats, False, False))
    half_lanes = -(-lanes // 256) * 128
    span = -(-(3 * (lanes // 4)) // 128) * 128 - lanes // 4 // 128 * 128

    def unet(which):
        return call(
            lambda *refs: unet_kernel(which, lats, breadth, *refs),
            (shape((c0, height * breadth), BF), shape((c0, variables), BF))[: 1 + which],
            [
                pltpu.VMEM((4, c0, lanes), BF),
                pltpu.VMEM((6 * 3 * c0, lanes), BF),
                pltpu.VMEM((4 * 3 * c0, half_lanes), BF),
                pltpu.VMEM((4 * 3 * c1, half_lanes), BF),
                pltpu.VMEM((6 * 6 * c0, span), BF),
            ],
            (half_x, half_y, far_x, far_y, enc_conv, down_conv.transpose(0, 2, 1), mid_conv)
            + (up_proj, unite_conv, out_proj.T)[: 2 + which],
            20,
            [vmem] * (9 + which),
        )

    swap = [(0, 1), (1, 0)]
    map_a = lax.ppermute(unet(0)[0], "section", swap)
    map_b, w_out = unet(1)
    map_b = lax.cond(
        crossing > 0, lambda v: lax.ppermute(v, "section", swap), lambda v: v, map_b
    )
    return call(
        project_kernel,
        shape((samples, variables, height, breadth), BF),
        [
            pltpu.VMEM((2, variables * height, breadth), F32),
            pltpu.VMEM((2, variables, height, breadth), BF),
            pltpu.SemaphoreType.DMA((2,)),
        ],
        (map_a, map_b, w_out),
        12,
        out_space=hbm,
    )


def solution(mesh):
    return jax.shard_map(
        shards,
        mesh=mesh,
        in_specs=(P("section", None, "lat", "lon"), P(), P(), P(), P(), P(), P(), P(), P()),
        out_specs=P("section", None, "lat", "lon"),
        check_vma=False,
    )
```

```python
import jax
import jax.numpy as jnp
from jax import lax
from jax.experimental import pallas as pl
from jax.experimental.pallas import tpu as pltpu
from jax.sharding import PartitionSpec as P

BF = jnp.bfloat16
F32 = jnp.float32
HALO = 8
LIMIT_ROWS = 52.7


def gelu_of_double(h):
    inner = h * (1.5957691216057308 + 0.285419265090401 * (h * h))
    return h + h * jnp.tanh(inner)


def halved(weights):
    return weights * jnp.asarray(0.5, BF)


def dot(a, b):
    return jnp.dot(a, b, preferred_element_type=F32)


def across(a, b):
    return lax.dot_general(a, b, (((0,), (0,)), ((), ())), preferred_element_type=F32)


def shift(x, by):
    n = x.shape[1]
    by = by % n
    if by == 0:
        return x
    return jnp.concatenate([x[:, by:], x[:, :by]], axis=1)


def swap_pairs(count, odd, periodic):
    pairs = []
    for low in range(1 if odd else 0, count, 2):
        high = low + 1
        if high >= count:
            if not periodic:
                continue
            high = 0
        pairs += [(low, high), (high, low)]
    return pairs


def rows_kernel(fields, picked, held, tall, sems):
    samples, variables, height, breadth = fields.shape
    loads = [pltpu.make_async_copy(fields.at[b], held.at[b], sems.at[b]) for b in range(samples)]
    for load in loads:
        load.start()
    for b in range(samples):
        loads[b].wait()
        tall[...] = held[b].astype(F32).reshape(variables * height, breadth)
        for i in range(height):
            picked[b, :, i * breadth : (i + 1) * breadth] = tall[pl.ds(i, variables, stride=height), :].astype(BF)


def stem_kernel(height, breadth, picked, w_in, stem, strip_x, strip_y):
    samples = picked.shape[0]
    odd = lax.axis_index("lon") % 2
    for b in range(samples):
        full = gelu_of_double(dot(halved(w_in[...]), picked[b])).astype(BF)
        stem[b] = full
        left = jnp.concatenate([full[:, i * breadth : i * breadth + HALO] for i in range(height)], axis=1)
        right = jnp.concatenate(
            [full[:, (i + 1) * breadth - HALO : (i + 1) * breadth] for i in range(height)], axis=1
        )
        strip_x[b] = jnp.where(odd == 1, left, right)
        strip_y[b] = jnp.where(odd == 1, right, left)


def widen_kernel(breadth, plan, stem, recv_x, recv_y, half_x, half_y):
    samples = stem.shape[0]
    turns = plan[...].astype(F32).reshape(1, 2 * samples)
    turn = lax.broadcasted_iota(jnp.int32, turns.shape, 1)
    first, last = (jnp.sum(jnp.where(turn == n, turns, 0.0)) for n in (0, 2 * samples - 1))
    leaving = jnp.where(lax.axis_index("section") == 0, last, first - samples)
    height = stem.shape[2] // breadth
    half = height // 2
    lon_odd = lax.axis_index("lon") % 2
    lat_odd = lax.axis_index("lat") % 2
    for b in range(samples):
        full = stem[b]
        from_x, from_y = recv_x[b], recv_y[b]
        left = jnp.where(lon_odd == 1, from_x, from_y)
        right = jnp.where(lon_odd == 1, from_y, from_x)
        halves = []
        for first in (0, half):
            pieces = []
            for m in range(4):
                for k in range(half // 4):
                    i = first + 4 * k + m
                    pieces += [
                        left[:, i * HALO : (i + 1) * HALO],
                        full[:, i * breadth : (i + 1) * breadth],
                        right[:, i * HALO : (i + 1) * HALO],
                    ]
            halves.append(jnp.concatenate(pieces, axis=1))
        slot = jnp.where(leaving == b, 0, 1)
        half_x[pl.ds(slot, 1)] = jnp.where(lat_odd == 1, halves[0], halves[1])[None]
        half_y[pl.ds(slot, 1)] = jnp.where(lat_odd == 1, halves[1], halves[0])[None]


def by_row(kernel):
    return jnp.concatenate([kernel[n] for n in range(kernel.shape[0])], axis=1)


def paired(kernel):
    flat = by_row(kernel)
    zeros = jnp.zeros((flat.shape[0], flat.shape[1] // 3), BF)
    return jnp.concatenate(
        [jnp.concatenate([flat, zeros], axis=1), jnp.concatenate([zeros, flat], axis=1)], axis=0
    )


def unet_kernel(which, lat_count, breadth, own_x, own_y, recv_x, recv_y, enc, down, mid, w_up, unite, *refs):
    if which == 1:
        w_out, merged, w_out_held = refs[:3]
        w_out_held[...] = w_out[...]
    else:
        merged = refs[0]
    quads, zz1, zz2, zz3, zz4 = refs[1 + 2 * which :]
    pitch = breadth + 2 * HALO
    lat = lax.axis_index("lat")
    even = lat % 2 == 0
    mine_x, mine_y, far_x, far_y = own_x[which], own_y[which], recv_x[which], recv_y[which]
    quads[0] = jnp.where(even, far_y, far_x)
    quads[1] = jnp.where(even, mine_y, mine_x)
    quads[2] = jnp.where(even, mine_x, mine_y)
    quads[3] = jnp.where(even, far_x, far_y)
    c0 = quads.shape[1]
    lanes = quads.shape[2]
    quarter = lanes // 4
    low_edge = lat == 0
    high_edge = lat == lat_count - 1

    def keep(width, low, high):
        lane = lax.broadcasted_iota(jnp.int32, (1, width), 1)
        drop = (low_edge & (lane < low)) | (high_edge & (lane >= high))
        return jnp.where(drop, 0.0, 1.0).astype(F32)

    full_keep = keep(lanes, quarter, lanes - quarter)
    planes = [
        jnp.concatenate([quads[s, :, m * quarter : (m + 1) * quarter] for s in range(4)], axis=1)
        for m in range(4)
    ]
    rows = [shift(planes[3], -pitch)] + planes + [shift(planes[0], pitch)]
    for j, row in enumerate(rows):
        base = j * 3 * c0
        zz1[base : base + c0] = shift(row, -1)
        zz1[base + c0 : base + 2 * c0] = row
        zz1[base + 2 * c0 : base + 3 * c0] = shift(row, 1)
    skip = []
    for q in range(2):
        out = dot(halved(paired(enc)), zz1[2 * q * 3 * c0 : (2 * q + 4) * 3 * c0])
        out = (gelu_of_double(out) * full_keep).astype(BF)
        skip += [out[:c0], out[c0:]]

    blocks = -(-lanes // 256)
    spare = blocks * 256 - lanes
    to_lane = lax.broadcasted_iota(jnp.int32, (512, 128), 1)
    from_lane = lax.broadcasted_iota(jnp.int32, (512, 128), 0) % 256
    gather = jnp.where(from_lane // 2 == to_lane, 0.25, 0.0).astype(BF)
    stacked = []
    for h in range(2):
        pair = [
            jnp.concatenate([skip[2 * h + e], jnp.zeros((c0, spare), BF)], axis=1) if spare else skip[2 * h + e]
            for e in range(2)
        ]
        for t in range(blocks):
            stacked.append(
                jnp.concatenate([pair[0][:, 256 * t : 256 * (t + 1)], pair[1][:, 256 * t : 256 * (t + 1)]], axis=1)
            )
    small = dot(jnp.concatenate(stacked, axis=0), gather).astype(BF)
    pooled = [
        jnp.concatenate([small[(h * blocks + t) * c0 : (h * blocks + t + 1) * c0] for t in range(blocks)], axis=1)
        for h in range(2)
    ]
    half_lanes = 128 * blocks
    half_pitch = pitch // 2
    half_keep = keep(half_lanes, quarter // 2, (lanes - quarter) // 2)

    def halves(scratch, source):
        width = source[0].shape[0]
        for j, row in enumerate(
            (shift(source[1], -half_pitch), source[0], source[1], shift(source[0], half_pitch))
        ):
            base = j * 3 * width
            scratch[base : base + width] = shift(row, -1)
            scratch[base + width : base + 2 * width] = row
            scratch[base + 2 * width : base + 3 * width] = shift(row, 1)

    halves(zz2, pooled)
    w_down = jnp.concatenate([down[n] for n in range(down.shape[0])], axis=0)
    deep = []
    for h in range(2):
        out = across(halved(w_down), zz2[h * 3 * c0 : (h + 3) * 3 * c0])
        deep.append((gelu_of_double(out) * half_keep).astype(BF))
    halves(zz3, deep)
    c1 = deep[0].shape[0]
    lifted = []
    for h in range(2):
        out = dot(halved(by_row(mid)), zz3[h * 3 * c1 : (h + 3) * 3 * c1])
        middle = (gelu_of_double(out) + deep[h].astype(F32)).astype(BF)
        lifted.append((dot(w_up[...], middle) * half_keep).astype(BF))
    wide_lane = lax.broadcasted_iota(jnp.int32, (128, 256), 1)
    thin_lane = lax.broadcasted_iota(jnp.int32, (128, 256), 0)
    spread = jnp.where(wide_lane // 2 == thin_lane, 1.0, 0.0).astype(BF)
    stacked = jnp.concatenate(
        [lifted[h][:, 128 * t : 128 * (t + 1)] for h in range(2) for t in range(blocks)], axis=0
    )
    large = dot(stacked, spread).astype(BF)
    raised = [
        jnp.concatenate([large[(h * blocks + t) * c0 : (h * blocks + t + 1) * c0] for t in range(blocks)], axis=1)
        for h in range(2)
    ]
    start = quarter // 128 * 128
    span = zz4.shape[1]
    lift_rows = [(raised[1], -pitch), (raised[0], 0), (raised[0], 0), (raised[1], 0), (raised[1], 0), (raised[0], pitch)]
    skip_rows = [(skip[3], -pitch)] + [(s, 0) for s in skip] + [(skip[0], pitch)]
    for j in range(6):
        for b in range(3):
            base = (3 * j + b) * 2 * c0
            row, move = lift_rows[j]
            at = start + move + b - 1
            zz4[base : base + c0] = row[:, at : at + span]
            row, move = skip_rows[j]
            zz4[base + c0 : base + 2 * c0] = row[:, at : at + span]
    joined = []
    for q in range(2):
        out = dot(halved(paired(unite)), zz4[2 * q * 6 * c0 : (2 * q + 4) * 6 * c0])
        out = gelu_of_double(out).astype(BF)
        joined += [out[:c0], out[c0:]]
    rest = quarter - start
    pieces = []
    for k in range(lanes // pitch // 2):
        for m in range(4):
            at = rest + k * pitch + HALO
            pieces.append(joined[m][:, at : at + breadth])
    merged[...] = jnp.concatenate(pieces, axis=1)


def project_kernel(map_a, map_b, w_out, out, tall, ready, sems):
    section = lax.axis_index("section")
    variables, height, breadth = out.shape[1:]
    stores = []
    for n, source in enumerate((map_b, map_a)):
        full = across(w_out[...], source[...])
        for i in range(height):
            tall[n, pl.ds(i, variables, stride=height), :] = full[:, i * breadth : (i + 1) * breadth]
        ready[n] = tall[n].astype(BF).reshape(variables, height, breadth)
        store = pltpu.make_async_copy(ready.at[n], out.at[section if n == 1 else 1 - section], sems.at[n])
        store.start()
        stores.append(store)
    for store in stores:
        store.wait()


def call(kernel, outs, scratch, args, mebibytes, spaces=None, out_space=None):
    vmem = pl.BlockSpec(memory_space=pltpu.VMEM)
    return pl.pallas_call(
        kernel,
        out_shape=outs,
        in_specs=spaces if spaces else [vmem] * len(args),
        out_specs=out_space or jax.tree.map(lambda _: vmem, outs),
        scratch_shapes=scratch,
        compiler_params=pltpu.CompilerParams(vmem_limit_bytes=int(mebibytes * 2**20)),
    )(*args)


def shards(fields_in, plan, in_proj, enc_conv, down_conv, mid_conv, up_proj, unite_conv, out_proj):
    samples, variables, height, breadth = fields_in.shape
    c0, c1 = in_proj.shape[0], up_proj.shape[1]
    sections, lats, lons = lax.axis_size("section"), lax.axis_size("lat"), lax.axis_size("lon")
    shape = jax.ShapeDtypeStruct
    lanes = height // 2 * (breadth + 2 * HALO)

    hbm, vmem, smem = (pl.BlockSpec(memory_space=s) for s in (pltpu.HBM, pltpu.VMEM, pltpu.SMEM))
    strip = shape((samples, c0, height * HALO), BF)
    picked = call(
        rows_kernel,
        shape((samples, variables, height * breadth), BF),
        [
            pltpu.VMEM((samples, variables, height, breadth), BF),
            pltpu.VMEM((variables * height, breadth), F32),
            pltpu.SemaphoreType.DMA((samples,)),
        ],
        (fields_in,),
        LIMIT_ROWS,
        [hbm],
    )
    stem, strip_x, strip_y = call(
        lambda *refs: stem_kernel(height, breadth, *refs),
        (shape((samples, c0, height * breadth), BF), strip, strip),
        [],
        (picked, in_proj),
        12,
    )
    recv_y = lax.ppermute(strip_y, "lon", swap_pairs(lons, True, True))
    recv_x = lax.ppermute(strip_x, "lon", swap_pairs(lons, False, True))
    half = shape((samples, c0, lanes), BF)
    crossing = (plan[samples - 1] >= samples).astype(jnp.int32)
    recv_x, recv_y, crossing = lax.optimization_barrier((recv_x, recv_y, crossing))
    half_x, half_y = call(
        lambda *refs: widen_kernel(breadth, *refs), (half, half), [], (plan, stem, recv_x, recv_y), 8
    )
    far_y = lax.ppermute(half_y, "lat", swap_pairs(lats, True, False))
    far_x = lax.ppermute(half_x, "lat", swap_pairs(lats, False, False))
    half_lanes = -(-lanes // 256) * 128
    span = -(-(3 * (lanes // 4)) // 128) * 128 - lanes // 4 // 128 * 128

    def unet(which):
        return call(
            lambda *refs: unet_kernel(which, lats, breadth, *refs),
            (shape((c0, height * breadth), BF), shape((c0, variables), BF))[: 1 + which],
            [
                pltpu.VMEM((4, c0, lanes), BF),
                pltpu.VMEM((6 * 3 * c0, lanes), BF),
                pltpu.VMEM((4 * 3 * c0, half_lanes), BF),
                pltpu.VMEM((4 * 3 * c1, half_lanes), BF),
                pltpu.VMEM((6 * 6 * c0, span), BF),
            ],
            (half_x, half_y, far_x, far_y, enc_conv, down_conv.transpose(0, 2, 1), mid_conv)
            + (up_proj, unite_conv, out_proj.T)[: 2 + which],
            20,
            [vmem] * (9 + which),
        )

    swap = [(0, 1), (1, 0)]
    map_a = lax.ppermute(unet(0)[0], "section", swap)
    map_b, w_out = unet(1)
    map_b = lax.cond(
        crossing > 0, lambda v: lax.ppermute(v, "section", swap), lambda v: v, map_b
    )
    return call(
        project_kernel,
        shape((samples, variables, height, breadth), BF),
        [
            pltpu.VMEM((2, variables * height, breadth), F32),
            pltpu.VMEM((2, variables, height, breadth), BF),
            pltpu.SemaphoreType.DMA((2,)),
        ],
        (map_a, map_b, w_out),
        12,
        out_space=hbm,
    )


def solution(mesh):
    return jax.shard_map(
        shards,
        mesh=mesh,
        in_specs=(P("section", None, "lat", "lon"), P(), P(), P(), P(), P(), P(), P(), P()),
        out_specs=P("section", None, "lat", "lon"),
        check_vma=False,
    )
```
